32 devices in a mesh: dp: 4 (over y, core), expert: 4 (over z), tensor: 2 (over x).
Axes of the slice: x: 2, y: 2, z: 4, core: 2. Of those that a mesh axis runs over, the one named last changes fastest.
Arguments:
- tokens: bfloat16 [256, 3072], P(('dp', 'expert')), may hold values from -45 to 45
- cotangent: bfloat16 [256, 3072], P(('dp', 'expert')), may hold values from -6 to 6
- gain: float32 [3072], replicated, may hold values from 0.5 to 1.5
- w_router: bfloat16 [3072, 4], replicated, may hold values from -0.109375 to 0.109375
- w_gate: bfloat16 [4, 3072, 9216], P('expert', None, 'tensor'), may hold values from -0.109375 to 0.109375
- w_up: bfloat16 [4, 3072, 9216], P('expert', None, 'tensor'), may hold values from -0.109375 to 0.109375
- w_down: bfloat16 [4, 9216, 3072], P('expert', 'tensor'), may hold values from -0.0625 to 0.0625
- expert_ids: int32 [256, 2], P(('dp', 'expert')), may hold values from 0 to 3, as said below
- slots: int32 [256, 2], P(('dp', 'expert')), may hold values from 0 to 7, as said below
Outputs:
- mixed: bfloat16 [256, 3072], P(('dp', 'expert'))
- grad_tokens: bfloat16 [256, 3072], P(('dp', 'expert'))
- grad_router: float32 [3072, 4], replicated
- grad_gain: float32 [3072], replicated
The draws below stay inside these ranges and needn't reach their ends.
Inputs may be any that keep to these rules, and one draw needn't show every extreme that they name: `expert_ids`: within each aligned block of 16 rows (one group), every expert is named exactly 8 times, and a row's two ids differ. Within each aligned block of 16 rows, the choices naming one expert hold its slots 0 to 7, each once.
All inputs are finite; a program needn't handle non-finite values.
Results may differ from the reference program's by a relative error of at most 0.0095.
Values may be sent and summed in bfloat16 or wider, within the bound.
No kernel may reach another device: no remote copies, remote signals or barrier semaphores. Data moves between devices by JAX's collectives and lax.ppermute only.
A program may use at most 128 MiB of HBM per device.

```python
import jax
import jax.numpy as jnp
from jax import lax

D = 3072
FF = 9216
TOK_DEV = 16
SUBS = 1
EXPERTS = 4
CAP = 8
GROUPS = 16
TOKENS = 256


def draw_tokens(key, part):
    base_key, row_key, column_key = jax.random.split(key, 3)
    base = jax.random.truncated_normal(base_key, -4.0, 4.0, (TOKENS, D), jnp.float32)
    row_scale = 10.0 ** jax.random.uniform(row_key, (TOKENS, 1), jnp.float32, -0.5, 0.5)
    column_scale = 10.0 ** jax.random.uniform(column_key, (1, D), jnp.float32, -0.5, 0.5)
    return (base * row_scale * column_scale).astype(jnp.bfloat16)


def group_routes(group_key):
    perm_key, shift_key, swap_key, rank_key = jax.random.split(group_key, 4)
    shuffled = jax.random.permutation(perm_key, TOK_DEV).astype(jnp.int32)
    first_ids = shuffled % EXPERTS
    round_index = shuffled // EXPERTS
    shift_by = jax.random.randint(shift_key, (TOK_DEV // EXPERTS,), 1, EXPERTS).astype(jnp.int32)
    second_ids = (first_ids + shift_by[round_index]) % EXPERTS
    swapped = jax.random.randint(swap_key, (TOK_DEV,), 0, 2).astype(jnp.int32)
    left = jnp.where(swapped == 1, second_ids, first_ids)
    right = jnp.where(swapped == 1, first_ids, second_ids)
    chosen_ids = jnp.stack([left, right], axis=1)
    ranking = jax.random.permutation(rank_key, 2 * TOK_DEV).astype(jnp.int32)
    flat_ids = chosen_ids.reshape(-1)
    same_expert = flat_ids[:, None] == flat_ids[None, :]
    earlier = ranking[None, :] < ranking[:, None]
    slot_ids = jnp.sum((same_expert & earlier).astype(jnp.int32), axis=1).reshape(TOK_DEV, 2)
    return (chosen_ids, slot_ids)


def route_tables(key):
    folded = jax.random.fold_in(key, 7)
    group_keys = jax.random.split(folded, TOKENS // TOK_DEV)
    chosen_ids, slot_ids = jax.vmap(group_routes)(group_keys)
    return (chosen_ids.reshape(TOKENS, 2).astype(jnp.int32), slot_ids.reshape(TOKENS, 2).astype(jnp.int32))


def draw_expert_ids(key, part):
    return route_tables(key)[0]


def draw_slots(key, part):
    return route_tables(key)[1]


def levels(own_key, dims, pieces, low, top_value):
    loudness = 1.0
    for dim, parts in pieces:
        steps = jax.random.uniform(jax.random.fold_in(jax.random.fold_in(own_key, 6), dim), (parts,), jnp.float32, low / len(pieces), top_value / len(pieces))
        loudness = loudness * jnp.repeat(jnp.exp(steps), dims[dim] // parts).reshape((-1,) + (1,) * (len(dims) - 1 - dim))
    return loudness


def scatter_about(rng, dims, spread, bound, cuts=(), held_as=jnp.bfloat16):
    result = jax.random.normal(rng, dims, jnp.float32) * spread
    if len(cuts) > 0:
        result = levels(rng, dims, cuts, -0.22, 0.18) * result
    return jnp.clip(result, min=-bound, max=bound).astype(held_as)


def setup_inputs(seed: int = 0) -> dict:
    streams_of = jax.random.split(jax.random.key(seed), 10)
    tokens = draw_tokens(jax.random.fold_in(streams_of[9], 71), 0)
    cotangent = scatter_about(streams_of[1], (TOKENS, D), 1.0, 6.0, ((0, 16),))
    gain = jnp.clip(1.0 + 0.1 * jax.random.normal(streams_of[2], (D,), jnp.float32), 0.5, 1.5)
    w_router = scatter_about(streams_of[3], (D, EXPERTS), D ** -0.5, 0.109375)
    w_gate = scatter_about(streams_of[4], (EXPERTS * SUBS, D, FF // SUBS), D ** -0.5, 0.109375, ((0, 4), (2, 2)))
    w_up = scatter_about(streams_of[5], (EXPERTS * SUBS, D, FF // SUBS), D ** -0.5, 0.109375, ((0, 4), (2, 2)))
    w_down = scatter_about(streams_of[6], (EXPERTS * SUBS, FF // SUBS, D), FF ** -0.5, 0.0625, ((0, 4), (1, 2)))
    expert_ids = draw_expert_ids(jax.random.fold_in(streams_of[9], 71), 0)
    slots = draw_slots(jax.random.fold_in(streams_of[9], 71), 0)
    return {"tokens": tokens, "cotangent": cotangent, "gain": gain, "w_router": w_router, "w_gate": w_gate, "w_up": w_up, "w_down": w_down, "expert_ids": expert_ids, "slots": slots}


epsilon = 1e-05

def reference(tokens, cotangent, gain, w_router, w_gate, w_up, w_down, expert_ids, slots):
    floats = tokens.astype(jnp.float32)
    inv_rms = lax.rsqrt(lax.optimization_barrier(jnp.mean(floats * floats, axis=1, keepdims=True)) + epsilon)
    normed = (floats * inv_rms * gain).astype(jnp.bfloat16)
    logits = jnp.dot(normed, w_router, preferred_element_type=jnp.float32)
    chosen_logits = jnp.take_along_axis(logits, expert_ids, axis=1)
    first_prob = jax.nn.sigmoid(chosen_logits[:, 0] - chosen_logits[:, 1])
    pair_probs = jnp.stack([first_prob, 1.0 - first_prob], axis=1)
    feature_width = tokens.shape[1]
    group_index = jnp.arange(TOKENS, dtype=jnp.int32) // TOK_DEV
    places = (group_index[:, None] * CAP + slots).astype(jnp.int32)
    expert_inputs = jnp.zeros((EXPERTS, GROUPS * CAP, feature_width), jnp.bfloat16)
    expert_inputs = expert_inputs.at[expert_ids, places].set(jnp.broadcast_to(normed[:, None, :], (TOKENS, 2, feature_width)))
    upstream = cotangent.astype(jnp.float32)
    sent_grads = (pair_probs[:, :, None] * upstream[:, None, :]).astype(jnp.bfloat16)
    expert_grads = jnp.zeros((EXPERTS, GROUPS * CAP, feature_width), jnp.bfloat16)
    expert_grads = expert_grads.at[expert_ids, places].set(sent_grads)
    hidden = w_gate.shape[2]
    gate_blocks = w_gate.reshape(EXPERTS, SUBS, feature_width, hidden)
    up_blocks = w_up.reshape(EXPERTS, SUBS, feature_width, hidden)
    down_blocks = w_down.reshape(EXPERTS, SUBS * hidden, feature_width)

    def one_expert(operand):
        rows_in, grads_in, gate_part, up_part, down_full = operand
        gate_full = jnp.transpose(gate_part, (1, 0, 2)).reshape(feature_width, SUBS * hidden)
        up_full = jnp.transpose(up_part, (1, 0, 2)).reshape(feature_width, SUBS * hidden)
        gate_pre = jnp.dot(rows_in, gate_full, preferred_element_type=jnp.float32)
        up_pre = jnp.dot(rows_in, up_full, preferred_element_type=jnp.float32)
        activated = (jax.nn.silu(gate_pre) * up_pre).astype(jnp.bfloat16)
        expert_out = jnp.dot(activated, down_full, preferred_element_type=jnp.float32)
        grad_act = jnp.dot(grads_in, down_full.T, preferred_element_type=jnp.float32)
        sigmoid_gate = jax.nn.sigmoid(gate_pre)
        grad_gate = (grad_act * up_pre * sigmoid_gate * (1.0 + gate_pre * (1.0 - sigmoid_gate))).astype(jnp.bfloat16)
        grad_up = (grad_act * jax.nn.silu(gate_pre)).astype(jnp.bfloat16)
        expert_back = jnp.dot(grad_gate, gate_full.T, preferred_element_type=jnp.float32) + jnp.dot(grad_up, up_full.T, preferred_element_type=jnp.float32)
        return (expert_out, expert_back)
    expert_out, expert_back = lax.map(one_expert, (expert_inputs, expert_grads, gate_blocks, up_blocks, down_blocks))
    chosen = expert_out[expert_ids, places]
    mixed = (floats + lax.optimization_barrier(jnp.sum(pair_probs[:, :, None] * chosen, axis=1))).astype(jnp.bfloat16)
    grad_mixture = lax.optimization_barrier(jnp.sum(expert_back[expert_ids, places], axis=1))
    grad_probs = lax.optimization_barrier(jnp.sum(upstream[:, None, :] * chosen, axis=2))
    grad_first = first_prob * (1.0 - first_prob) * (grad_probs[:, 0] - grad_probs[:, 1])
    columns = jnp.arange(EXPERTS, dtype=jnp.int32)[None, :]
    grad_logits = grad_first[:, None] * ((expert_ids[:, 0:1] == columns).astype(jnp.float32) - (expert_ids[:, 1:2] == columns).astype(jnp.float32))
    grad_router = jnp.dot(normed.astype(jnp.float32).T, grad_logits, precision=lax.Precision.HIGHEST)
    grad_normed = grad_mixture + jnp.dot(grad_logits, w_router.astype(jnp.float32).T, precision=lax.Precision.HIGHEST)
    grad_gain = lax.optimization_barrier(jnp.sum(grad_normed * floats * inv_rms, axis=0))
    grad_scaled = grad_normed * gain
    cubed = inv_rms * inv_rms * inv_rms
    grad_tokens = (upstream + inv_rms * grad_scaled - floats * cubed * lax.optimization_barrier(jnp.mean(grad_scaled * floats, axis=1, keepdims=True))).astype(jnp.bfloat16)
    return (mixed, grad_tokens, grad_router, grad_gain)
```

```python
import functools

import jax
import jax.numpy as jnp
from jax import lax
from jax.experimental import pallas as pl
from jax.experimental.pallas import tpu as pltpu
from jax.sharding import PartitionSpec as P

epsilon = 1e-05
MIB = 1 << 20
VMEM = pl.BlockSpec(memory_space=pltpu.VMEM)
SMEM = pl.BlockSpec(memory_space=pltpu.SMEM)
HBM = pl.BlockSpec(memory_space=pltpu.HBM)
NN = (((1,), (0,)), ((), ()))
NT = (((1,), (1,)), ((), ()))
TN = (((0,), (0,)), ((), ()))


def mm(a, b, dims):
    return lax.dot_general(a, b, dims, preferred_element_type=jnp.float32)


def shape(dims, dtype):
    return jax.ShapeDtypeStruct(dims, dtype)


def call(body, ins, in_specs, outs, scratch=(), limit=8, flops=0, moved=0):
    return pl.pallas_call(
        body,
        in_specs=in_specs,
        out_specs=[VMEM] * len(outs),
        out_shape=outs,
        scratch_shapes=scratch,
        compiler_params=pltpu.CompilerParams(vmem_limit_bytes=limit * MIB),
        cost_estimate=pl.CostEstimate(flops=flops, bytes_accessed=moved, transcendentals=0),
    )(*ins)


def piece(size):
    for width in (256, 128):
        if size % width == 0:
            return width
    return size


def one_hot(index_ref, column, rows):
    places = lax.broadcasted_iota(jnp.int32, (index_ref.shape[0], rows), 1)
    return index_ref[:, column : column + 1] == places


def pack_tokens(index_ref, tokens_ref, *refs):
    rows = len(refs) * refs[0].shape[0]
    select = (one_hot(index_ref, 0, rows) | one_hot(index_ref, 1, rows)).astype(jnp.bfloat16)
    split(mm(select, tokens_ref[...], TN), refs)


def route_grads(index_ref, ids_ref, tokens_ref, cotangent_ref, gain_ref, router_ref, *refs):
    *rows_refs, probs_ref, inv_ref, normed_ref = refs
    rows = len(rows_refs) * rows_refs[0].shape[0]
    floats = tokens_ref[...].astype(jnp.float32)
    inv = lax.rsqrt(jnp.mean(floats * floats, axis=1, keepdims=True) + epsilon)
    normed = (floats * inv * gain_ref[...]).astype(jnp.bfloat16)
    logits = mm(normed, router_ref[...], NN)
    experts = logits.shape[1]
    first = jnp.sum(jnp.where(one_hot(ids_ref, 0, experts), logits, 0.0), axis=1, keepdims=True)
    second = jnp.sum(jnp.where(one_hot(ids_ref, 1, experts), logits, 0.0), axis=1, keepdims=True)
    prob = jax.nn.sigmoid(first - second)
    upstream = cotangent_ref[...].astype(jnp.float32)
    sent_first = (prob * upstream).astype(jnp.bfloat16)
    sent_second = ((1.0 - prob) * upstream).astype(jnp.bfloat16)
    packed = mm(one_hot(index_ref, 0, rows).astype(jnp.bfloat16), sent_first, TN)
    packed += mm(one_hot(index_ref, 1, rows).astype(jnp.bfloat16), sent_second, TN)
    split(packed, rows_refs)
    probs_ref[...] = jnp.broadcast_to(prob, probs_ref.shape)
    inv_ref[...] = jnp.broadcast_to(inv, inv_ref.shape)
    normed_ref[...] = normed


def stack(refs):
    return jnp.concatenate([ref[...].astype(jnp.float32) for ref in refs], axis=0)


def forward(count, part_ref, *refs):
    tokens_refs = refs[:count]
    gain_ref, gate_ref, up_ref = refs[count : count + 3]
    act_ref, slope_ref, silu_ref, inv_ref, gate_here, up_here, sems = refs[count + 3 :]
    inner = act_ref.shape[1]
    width = piece(inner)
    copies = []
    for step in range(inner // width):
        here = pl.ds(step * width, width)
        there = pl.ds(pl.multiple_of(part_ref[0] * inner + step * width, width), width)
        pair = [
            pltpu.make_async_copy(ref.at[:, there], out.at[:, here], sems.at[2 * step + side])
            for side, (ref, out) in enumerate(((gate_ref, gate_here), (up_ref, up_here)))
        ]
        for copy in pair:
            copy.start()
        copies.append(pair)
    floats = stack(tokens_refs)
    inv = lax.rsqrt(jnp.mean(floats * floats, axis=1, keepdims=True) + epsilon)
    inv_ref[...] = jnp.broadcast_to(inv, inv_ref.shape)
    normed = (floats * inv * gain_ref[...]).astype(jnp.bfloat16)
    for step in range(inner // width):
        span = pl.ds(step * width, width)
        copies[step][0].wait()
        gate = mm(normed, gate_here[:, span], NN)
        copies[step][1].wait()
        up = mm(normed, up_here[:, span], NN)
        sigmoid = jax.nn.sigmoid(gate)
        silu = gate * sigmoid
        act_ref[:, span] = (silu * up).astype(jnp.bfloat16)
        slope_ref[span, :] = (up * sigmoid * (1.0 + gate * (1.0 - sigmoid))).T
        silu_ref[span, :] = silu.T


def middle(count, part_ref, *refs):
    act_ref, slope_ref, silu_ref, down_ref = refs[:4]
    grads_refs = refs[4 : 4 + count]
    *value_refs, gate_ref, up_ref, total_ref, down_here, sems = refs[4 + count :]
    inner = down_here.shape[0]
    height = piece(inner)
    copies = []
    for step in range(inner // height):
        there = pl.ds(pl.multiple_of(part_ref[0] * inner + step * height, height), height)
        copy = pltpu.make_async_copy(
            down_ref.at[there, :], down_here.at[pl.ds(step * height, height), :], sems.at[step]
        )
        copy.start()
        copies.append(copy)
    grads = stack(grads_refs).astype(jnp.bfloat16)
    for step in range(inner // height):
        span = pl.ds(step * height, height)
        copies[step].wait()
        value = mm(act_ref[:, span], down_here[span, :], NN)
        total_ref[...] = value if step == 0 else total_ref[...] + value
        grad_act = mm(down_here[span, :], grads, NT)
        gate_ref[span, :] = (grad_act * slope_ref[span, :]).astype(jnp.bfloat16)
        up_ref[span, :] = (grad_act * silu_ref[span, :]).astype(jnp.bfloat16)
    rows = value_refs[0].shape[0]
    for part, value_ref in enumerate(value_refs):
        value_ref[...] = total_ref[pl.ds(part * rows, rows), :].astype(value_ref.dtype)


def backward(count, *refs):
    gate_grad_ref, up_grad_ref, gate_ref, up_ref, inv_ref = refs[:5]
    tokens_refs = refs[5 : 5 + count]
    *value_refs, gain_ref = refs[5 + count :]
    rows = value_refs[0].shape[0]
    height = piece(gate_ref.shape[0])
    for start in range(0, gate_ref.shape[0], height):
        span = pl.ds(start, height)
        back = mm(gate_ref[span, :], gate_grad_ref[...], NN) + mm(up_ref[span, :], up_grad_ref[...], NN)
        back = back.T
        for part, value_ref in enumerate(value_refs):
            value_ref[:, span] = back[part * rows : (part + 1) * rows].astype(value_ref.dtype)
        floats = jnp.concatenate([ref[:, span].astype(jnp.float32) for ref in tokens_refs], axis=0)
        gain_ref[:, span] = jnp.sum(back * (floats * inv_ref[:, :1]), axis=0, keepdims=True)


def split(value, refs):
    rows = refs[0].shape[0]
    for place, ref in enumerate(refs):
        ref[...] = value[place * rows : (place + 1) * rows].astype(ref.dtype)


def add_pair(own_ref, other_ref, *refs):
    split(own_ref[...] + other_ref[...].astype(jnp.float32), refs)


def mix_rows(index_ref, probs_ref, cotangent_ref, *refs):
    *rows_refs, mix_ref, score_ref = refs
    rows = stack(rows_refs).astype(jnp.bfloat16)
    first = mm(one_hot(index_ref, 0, rows.shape[0]).astype(jnp.bfloat16), rows, NN)
    second = mm(one_hot(index_ref, 1, rows.shape[0]).astype(jnp.bfloat16), rows, NN)
    prob = probs_ref[:, :1]
    mix_ref[...] = (prob * first + (1.0 - prob) * second).astype(jnp.bfloat16)
    score = jnp.sum(cotangent_ref[...].astype(jnp.float32) * (first - second), axis=1, keepdims=True)
    score_ref[...] = jnp.broadcast_to(score, score_ref.shape)


def sum_rows(index_ref, *refs):
    *rows_refs, out_ref = refs
    rows = stack(rows_refs).astype(jnp.bfloat16)
    select = (one_hot(index_ref, 0, rows.shape[0]) | one_hot(index_ref, 1, rows.shape[0])).astype(jnp.bfloat16)
    out_ref[...] = mm(select, rows, NN).astype(jnp.bfloat16)


def finish_values(share, ids_ref, tokens_ref, mine_ref, other_ref, score_ref, other_score_ref, probs_ref, inv_ref, normed_ref, router_ref, mixed_ref, term_ref, parts_ref):
    floats = tokens_ref[...].astype(jnp.float32)
    mix = mine_ref[...].astype(jnp.float32) + other_ref[...].astype(jnp.float32)
    mixed_ref[...] = (floats + mix).astype(jnp.bfloat16)
    prob = probs_ref[:, :1]
    grad_first = prob * (1.0 - prob) * (score_ref[:, :1] + other_score_ref[:, :1])
    experts = router_ref.shape[0]
    grad_logits = jnp.where(one_hot(ids_ref, 0, experts), grad_first, 0.0)
    grad_logits -= jnp.where(one_hot(ids_ref, 1, experts), grad_first, 0.0)
    normed = normed_ref[...].astype(jnp.float32)
    term = jnp.zeros(floats.shape, jnp.float32)
    for expert in range(experts):
        column = grad_logits[:, expert : expert + 1]
        term += column * router_ref[expert : expert + 1, :].astype(jnp.float32)
        parts_ref[expert : expert + 1, :] = share * jnp.sum(column * normed, axis=0, keepdims=True)
    term_ref[...] = term
    local = jnp.sum(term * floats * inv_ref[:, :1], axis=0, keepdims=True)
    parts_ref[experts : experts + 1, :] = share * local


def finish_grads(tokens_ref, cotangent_ref, gain_ref, mine_ref, other_ref, term_ref, inv_ref, out_ref):
    floats = tokens_ref[...].astype(jnp.float32)
    inv = inv_ref[:, :1]
    grad_normed = mine_ref[...].astype(jnp.float32) + other_ref[...].astype(jnp.float32) + term_ref[...]
    grad_scaled = grad_normed * gain_ref[...]
    mean = jnp.mean(grad_scaled * floats, axis=1, keepdims=True)
    out_ref[...] = (
        cotangent_ref[...].astype(jnp.float32) + inv * grad_scaled - floats * (inv * inv * inv) * mean
    ).astype(jnp.bfloat16)


def swap(value, axis):
    size = lax.axis_size(axis)
    return lax.ppermute(value, axis, [(i, i ^ 1) for i in range(size)])


def sum_over(value, axis):
    size = lax.axis_size(axis)
    if size == 1:
        return value, jnp.zeros_like(value)
    if size == 2:
        return value, swap(value, axis)
    total = lax.psum(value.astype(jnp.float32), axis)
    return total.astype(value.dtype), jnp.zeros_like(value)


def trade(blocks, copies):
    if len(blocks) > 1:
        size = len(blocks)
        pairs = [[(i, i ^ step) for i in range(size)] for step in range(size)]
        return [blocks[0]] + [lax.ppermute(blocks[step], "expert", pairs[step]) for step in range(1, size)]
    size = lax.axis_size("expert")
    width = blocks[0].shape[1]
    if copies:
        experts = size // copies
        rows = blocks[0].reshape(experts, 1, -1, width)
        rows = jnp.broadcast_to(rows, (experts, copies) + rows.shape[2:])
    else:
        rows = blocks[0]
    rows = rows.reshape(size, -1, width)
    return [lax.all_to_all(rows, "expert", split_axis=0, concat_axis=0, tiled=True).reshape(-1, width)]


def bring_back(blocks, copies, experts):
    back = trade(blocks, 0)
    if copies > 1:
        rows = back[0].reshape(experts, copies, -1, back[0].shape[1]).astype(jnp.float32)
        back = [jnp.sum(rows, axis=1).reshape(-1, rows.shape[3]).astype(jnp.bfloat16)]
    return back


def all_sum(value, axes):
    count = 1
    for axis in axes:
        count *= lax.axis_size(axis)
    if value.size % count:
        return lax.psum(value, axes)
    blocks = value.reshape(count, -1)
    mine = lax.all_to_all(blocks, axes, split_axis=0, concat_axis=0, tiled=True)
    total = jnp.sum(mine, axis=0, keepdims=True)
    spread = jnp.broadcast_to(total, blocks.shape)
    return lax.all_to_all(spread, axes, split_axis=0, concat_axis=0, tiled=True).reshape(value.shape)


def layer(tokens, cotangent, gain, w_router, w_gate, w_up, w_down, expert_ids, slots):
    experts = w_router.shape[1]
    axis = lax.axis_size("expert")
    copies = axis // experts
    token_count, width = tokens.shape
    rows = 2 * token_count
    capacity = rows // experts
    hidden = w_gate.shape[2]
    parts = 2 if lax.axis_size("dp") % 2 == 0 and hidden % 256 == 0 else 1
    inner = hidden // parts
    paired = copies == 1 and axis in (2, 4, 8) and capacity % 8 == 0
    owner = expert_ids ^ lax.axis_index("expert") if paired else expert_ids
    index = owner * capacity + slots
    part = (lax.axis_index("dp") % parts).astype(jnp.int32).reshape(1)
    gain_row = gain.reshape(1, width)
    bf16, f32 = jnp.bfloat16, jnp.float32
    sends = [shape((capacity, width), bf16)] * experts if paired else [shape((rows, width), bf16)]
    count = axis * capacity
    all_rows = parts * count
    backs_shape = [shape((capacity, width), bf16)] * experts if paired else [shape((count, width), bf16)]

    gate_there, up_there, down_there = (
        pltpu.with_memory_space_constraint(w[0], pltpu.HBM) for w in (w_gate, w_up, w_down)
    )
    packed = call(pack_tokens, (index, tokens), [VMEM] * 2, sends)
    inputs = trade(packed, copies)
    *sent, probs, inv, normed = call(
        route_grads,
        (index, expert_ids, tokens, cotangent, gain_row, w_router),
        [VMEM] * 6,
        sends + [shape((token_count, 128), f32), shape((token_count, 128), f32), shape((token_count, width), bf16)],
    )
    grads = trade(sent, copies)
    if parts == 2:
        inputs = inputs + [swap(block, "dp") for block in inputs]
        grads = grads + [swap(block, "dp") for block in grads]
    pieces = len(inputs)
    steps = inner // piece(inner)
    act, slope, silu, inv_rows, gate_here, up_here = call(
        functools.partial(forward, pieces),
        (part, *inputs, gain_row, gate_there, up_there),
        [SMEM] + [VMEM] * (pieces + 1) + [HBM] * 2,
        [
            shape((all_rows, inner), bf16),
            shape((inner, all_rows), f32),
            shape((inner, all_rows), f32),
            shape((all_rows, 128), f32),
            pltpu.VMEM((width, inner), bf16),
            pltpu.VMEM((width, inner), bf16),
        ],
        [pltpu.SemaphoreType.DMA((2 * steps,))],
        flops=4 * all_rows * width * inner,
        moved=4 * width * inner,
    )
    value_shapes = [shape((count, width), f32)] + [shape((count, width), bf16)] * (parts - 1)
    *values, gate_grad, up_grad = call(
        functools.partial(middle, pieces),
        (part, act, slope, silu, down_there, *grads),
        [SMEM] + [VMEM] * 3 + [HBM] + [VMEM] * pieces,
        value_shapes + [shape((inner, all_rows), bf16)] * 2,
        [pltpu.VMEM((all_rows, width), f32), pltpu.VMEM((inner, width), bf16), pltpu.SemaphoreType.DMA((steps,))],
        limit=20,
        flops=4 * all_rows * width * inner,
        moved=2 * width * inner,
    )
    gate_here, up_here = (pltpu.with_memory_space_constraint(w, pltpu.VMEM) for w in (gate_here, up_here))
    *backs, gain_part = call(
        functools.partial(backward, pieces),
        (gate_grad, up_grad, gate_here, up_here, inv_rows, *inputs),
        [VMEM] * (5 + pieces),
        value_shapes + [shape((1, width), f32)],
        flops=4 * all_rows * width * inner,
        moved=4 * width * inner,
    )

    def home(pieces):
        if parts == 2:
            mine = call(add_pair, (pieces[0], swap(pieces[1], "dp")), [VMEM] * 2, backs_shape)
        else:
            mine = [pieces[0].astype(bf16)] if not paired else [
                pieces[0][i * capacity : (i + 1) * capacity].astype(bf16) for i in range(experts)
            ]
        return bring_back(mine, copies, experts)

    value_rows = home(values)
    mix, score = call(
        mix_rows,
        (index, probs, cotangent, *value_rows),
        [VMEM] * (3 + len(value_rows)),
        [shape((token_count, width), bf16), shape((token_count, 128), f32)],
    )
    mix, other_mix = sum_over(mix, "tensor")
    score, other_score = sum_over(score, "tensor")
    mixed, term, local = call(
        functools.partial(finish_values, 1.0 / lax.axis_size("tensor")),
        (expert_ids, tokens, mix, other_mix, score, other_score, probs, inv, normed, w_router.T),
        [VMEM] * 10,
        [shape((token_count, width), bf16), shape((token_count, width), f32), shape((experts + 1, width), f32)],
    )
    back_rows = home(backs)
    (back,) = call(sum_rows, (index, *back_rows), [VMEM] * (1 + len(back_rows)), [shape((token_count, width), bf16)])
    back, other_back = sum_over(back, "tensor")
    (grad_tokens,) = call(
        finish_grads,
        (tokens, cotangent, gain_row, back, other_back, term, inv),
        [VMEM] * 7,
        [shape((token_count, width), bf16)],
    )
    local = jnp.concatenate([local[:experts], local[experts:] + gain_part], axis=0)
    total = all_sum(local, ("dp", "expert", "tensor"))
    return (mixed, grad_tokens, total[:experts].T, total[experts])


def solution(mesh):
    return jax.shard_map(
        layer,
        mesh=mesh,
        in_specs=(
            P(("dp", "expert"), None),
            P(("dp", "expert"), None),
            P(),
            P(),
            P("expert", None, "tensor"),
            P("expert", None, "tensor"),
            P("expert", "tensor", None),
            P(("dp", "expert"), None),
            P(("dp", "expert"), None),
        ),
        out_specs=(P(("dp", "expert"), None), P(("dp", "expert"), None), P(), P()),
        check_vma=False,
    )
```

```python
import functools

import jax
import jax.numpy as jnp
from jax import lax
from jax.experimental import pallas as pl
from jax.experimental.pallas import tpu as pltpu
from jax.sharding import PartitionSpec as P


epsilon = 1e-05
MIB = 1 << 20
VMEM = pl.BlockSpec(memory_space=pltpu.VMEM)
SMEM = pl.BlockSpec(memory_space=pltpu.SMEM)
HBM = pl.BlockSpec(memory_space=pltpu.HBM)
NN = (((1,), (0,)), ((), ()))
NT = (((1,), (1,)), ((), ()))
TN = (((0,), (0,)), ((), ()))


def mm(a, b, dims):
    return lax.dot_general(a, b, dims, preferred_element_type=jnp.float32)


def shape(dims, dtype):
    return jax.ShapeDtypeStruct(dims, dtype)


def call(body, ins, in_specs, outs, scratch=(), limit=3, flops=0, moved=0):
    return pl.pallas_call(
        body,
        in_specs=in_specs,
        out_specs=[VMEM] * len(outs),
        out_shape=outs,
        scratch_shapes=scratch,
        compiler_params=pltpu.CompilerParams(vmem_limit_bytes=limit * MIB),
        cost_estimate=pl.CostEstimate(flops=flops, bytes_accessed=moved, transcendentals=0),
    )(*ins)


def piece(size):
    for width in (256, 128):
        if size % width == 0:
            return width
    return size


def load_all(pairs, sems):
    copies = [pltpu.make_async_copy(src, dst, sems.at[i]) for i, (src, dst) in enumerate(pairs)]
    for copy in copies:
        copy.start()
    for copy in copies:
        copy.wait()


def column(row):
    size = row.shape[1]
    across = lax.broadcasted_iota(jnp.int32, (size, size), 0)
    along = lax.broadcasted_iota(jnp.int32, (size, size), 1)
    return jnp.sum(jnp.where(across == along, row, 0.0), axis=1, keepdims=True)


def prepare(experts, capacity, paired, places_ref, ids_any, slots_any, tokens_any, cotangent_any, gain_any, router_any, *refs):
    outs = refs[: experts if paired else 2]
    first_ref, second_ref, probs_ref, inv_ref, signs_ref, normed_ref = refs[len(outs) : len(outs) + 6]
    tokens_ref, cotangent_ref, gain_ref, router_ref, ids_ref, slots_ref, sems = refs[len(outs) + 6 :]
    load_all(
        (
            (ids_any, ids_ref),
            (slots_any, slots_ref),
            (tokens_any, tokens_ref),
            (cotangent_any, cotangent_ref),
            (gain_any, gain_ref),
            (router_any, router_ref),
        ),
        sems,
    )
    rows = experts * capacity
    ids = ids_ref[...]
    owner = (ids ^ places_ref[0]) if paired else ids
    index = owner * capacity + slots_ref[...]
    places = lax.broadcasted_iota(jnp.int32, (rows, index.shape[1]), 0)
    first = places == index[0:1, :]
    second = places == index[1:2, :]
    first_ref[...] = first.astype(jnp.bfloat16)
    second_ref[...] = second.astype(jnp.bfloat16)
    select = (first | second).astype(jnp.bfloat16)
    tokens = tokens_ref[...]
    inputs = mm(select, tokens, NN)
    floats = tokens.astype(jnp.float32)
    inv = lax.rsqrt(jnp.mean(floats * floats, axis=1, keepdims=True) + epsilon)
    normed = (floats * inv * gain_ref[...]).astype(jnp.bfloat16)
    logits = mm(router_ref[...], normed, NT)
    names = lax.broadcasted_iota(jnp.int32, (experts, ids.shape[1]), 0)
    signs = (names == ids[0:1, :]).astype(jnp.float32) - (names == ids[1:2, :]).astype(jnp.float32)
    prob = jax.nn.sigmoid(jnp.sum(signs * logits, axis=0, keepdims=True))
    weights = jnp.sum(jnp.where(first, prob, 0.0) + jnp.where(second, 1.0 - prob, 0.0), axis=1, keepdims=True)
    grads = weights * mm(select, cotangent_ref[...], NN)
    if paired:
        for expert, ref in enumerate(outs):
            mine = slice(expert * capacity, (expert + 1) * capacity)
            ref[...] = jnp.concatenate([inputs[mine], grads[mine]], axis=0).astype(jnp.bfloat16)
    else:
        outs[0][...] = inputs.astype(jnp.bfloat16)
        outs[1][...] = grads.astype(jnp.bfloat16)
    probs_ref[...] = jnp.broadcast_to(column(prob), probs_ref.shape)
    inv_ref[...] = jnp.broadcast_to(inv, inv_ref.shape)
    normed_ref[...] = normed
    for expert in range(experts):
        signs_ref[:, expert : expert + 1] = column(signs[expert : expert + 1, :])


def fetch(places_ref, gate_ref, gate_out, sems):
    width = gate_out.shape[1]
    columns = pl.ds(pl.multiple_of(places_ref[1] * width, width), width)
    load_all(((gate_ref.at[:, columns], gate_out),), sems)


def stack(refs, paired=False, half=0):
    values = []
    for ref in refs:
        value = ref[...].astype(jnp.float32)
        if paired:
            rows = value.shape[0] // 2
            value = value[half * rows : (half + 1) * rows]
        values.append(value)
    return jnp.concatenate(values, axis=0)


def split(value, refs):
    rows = refs[0].shape[0]
    for place, ref in enumerate(refs):
        ref[...] = value[place * rows : (place + 1) * rows].astype(ref.dtype)


MIDDLE_FLIGHT = 3


def forward(count, paired, places_ref, *refs):
    tokens_refs = refs[:count]
    gain_ref, gate_ref, up_any, act_ref, slope_ref, silu_ref, scaled_ref, up_ref, sems = refs[count:]
    inner = act_ref.shape[1]
    width = piece(inner)
    copies = []
    for step in range(inner // width):
        there = pl.ds(pl.multiple_of(places_ref[1] * inner + step * width, width), width)
        here = up_ref.at[:, pl.ds(step * width, width)]
        copies.append(pltpu.make_async_copy(up_any.at[:, there], here, sems.at[step]))
        copies[step].start()
    floats = stack(tokens_refs, paired, 0)
    inv = lax.rsqrt(jnp.mean(floats * floats, axis=1, keepdims=True) + epsilon)
    scaled = floats * inv
    scaled_ref[...] = scaled
    normed = (scaled * gain_ref[...]).astype(jnp.bfloat16)
    for step in range(inner // width):
        span = pl.ds(step * width, width)
        gate = mm(normed, gate_ref[:, span], NN)
        copies[step].wait()
        up = mm(normed, up_ref[:, span], NN)
        sigmoid = jax.nn.sigmoid(gate)
        silu = gate * sigmoid
        act_ref[:, span] = (silu * up).astype(jnp.bfloat16)
        slope_ref[span, :] = (up * sigmoid * (1.0 + gate * (1.0 - sigmoid))).T
        silu_ref[span, :] = silu.T


def middle(count, paired, places_ref, act_ref, slope_ref, silu_ref, down_any, *refs):
    *value_refs, gate_ref, up_ref, total_ref, down_ref, sems = refs[count:]
    slots, height, _ = down_ref.shape
    inner = act_ref.shape[1]
    steps = inner // height

    def copy(step):
        there = pl.ds(pl.multiple_of(places_ref[1] * inner + step * height, height), height)
        return pltpu.make_async_copy(down_any.at[there, :], down_ref.at[step % slots], sems.at[step % slots])

    ahead = min(slots, steps) - 1
    for step in range(ahead):
        copy(step).start()
    grads = stack(refs[:count], paired, 1).T.astype(jnp.bfloat16)
    for step in range(steps):
        span = pl.ds(step * height, height)
        copy(step).wait()
        if step + ahead < steps:
            copy(step + ahead).start()
        down = down_ref.at[step % slots]
        grad_act = mm(down[...], grads, NN)
        value = mm(act_ref[:, span], down[...], NN)
        total_ref[...] = value if step == 0 else total_ref[...] + value
        gate_ref[span, :] = (grad_act * slope_ref[span, :]).astype(jnp.bfloat16)
        up_ref[span, :] = (grad_act * silu_ref[span, :]).astype(jnp.bfloat16)
    split(total_ref[...], value_refs)


def backward(gate_grad_ref, up_grad_ref, gate_ref, up_ref, scaled_ref, *refs):
    *value_refs, gain_ref = refs
    rows = value_refs[0].shape[0]
    height = piece(gate_ref.shape[0])
    for start in range(0, gate_ref.shape[0], height):
        span = pl.ds(start, height)
        back = mm(gate_ref[span, :], gate_grad_ref[...], NN) + mm(up_ref[span, :], up_grad_ref[...], NN)
        back = back.T
        for part, value_ref in enumerate(value_refs):
            value_ref[:, span] = back[part * rows : (part + 1) * rows].astype(value_ref.dtype)
        gain_ref[:, span] = jnp.sum(back * scaled_ref[:, span], axis=0, keepdims=True)


def add_pair(own_ref, other_ref, *refs):
    split(own_ref[...] + other_ref[...].astype(jnp.float32), refs)


def round_own(own_ref, *refs):
    split(own_ref[...], refs)


def mix_values(first_ref, second_ref, probs_ref, inv_ref, signs_ref, normed_ref, tokens_ref, cotangent_ref, router_ref, gain_part_ref, *refs):
    *rows_refs, mix_ref, sums_ref = refs
    rows = stack(rows_refs).astype(jnp.bfloat16)
    first = mm(first_ref[...], rows, TN)
    second = mm(second_ref[...], rows, TN)
    width = first.shape[1]
    prob = probs_ref[:, :1]
    mix_ref[:, :width] = (prob * first + (1.0 - prob) * second).astype(jnp.bfloat16)
    score = jnp.sum(cotangent_ref[...].astype(jnp.float32) * (first - second), axis=1, keepdims=True)
    coarse = score.astype(jnp.bfloat16)
    fine = (score - coarse.astype(jnp.float32)).astype(jnp.bfloat16)
    mix_ref[:, width:] = jnp.zeros((mix_ref.shape[0], mix_ref.shape[1] - width), jnp.bfloat16)
    mix_ref[:, width : width + 1] = coarse
    mix_ref[:, width + 1 : width + 2] = fine
    grad_first = prob * (1.0 - prob) * score
    normed = normed_ref[...].astype(jnp.float32)
    term = jnp.zeros(first.shape, jnp.float32)
    experts = router_ref.shape[0]
    sums = []
    for expert in range(experts):
        column = grad_first * signs_ref[:, expert : expert + 1]
        term += column * router_ref[expert : expert + 1, :].astype(jnp.float32)
        sums.append(jnp.sum(column * normed, axis=0, keepdims=True))
    scaled = tokens_ref[...].astype(jnp.float32) * inv_ref[:, :1]
    sums.append(jnp.sum(term * scaled, axis=0, keepdims=True) + gain_part_ref[...])
    spread(sums, sums_ref)


def spread(rows, out_ref):
    lanes = 128
    across = out_ref.shape[1] // lanes
    place = 0
    for row in rows:
        for start in range(0, row.shape[1], lanes):
            top, left = place // across, place % across * lanes
            out_ref[top : top + 1, left : left + lanes] = row[:, start : start + lanes]
            place += 1
    while place < out_ref.shape[0] * across:
        top, left = place // across, place % across * lanes
        out_ref[top : top + 1, left : left + lanes] = jnp.zeros((1, lanes), jnp.float32)
        place += 1


def unpack(sums, router_ref, gain_ref):
    lanes = 128
    across = sums.shape[1] // lanes
    steps = gain_ref.shape[1] // lanes
    experts = router_ref.shape[0]
    for expert in range(experts + 1):
        out_ref, row = (router_ref, expert) if expert < experts else (gain_ref, 0)
        for step in range(steps):
            place = expert * steps + step
            top, left = place // across, place % across * lanes
            value = sums[top : top + 1, left : left + lanes]
            out_ref[row : row + 1, step * lanes : (step + 1) * lanes] = value


def gather_sums(sums_ref, router_ref, gain_ref):
    unpack(sums_ref, router_ref, gain_ref)


def add_all(own_ref, other_ref, sums_ref, other_sums_ref, *refs):
    rows = refs[0].shape[0]
    width = own_ref.shape[1]
    total = own_ref[...] + other_ref[...].astype(jnp.float32)
    sums = (sums_ref[...] + other_sums_ref[...]).astype(jnp.bfloat16)
    for place, ref in enumerate(refs):
        ref[:, :width] = total[place * rows : (place + 1) * rows].astype(jnp.bfloat16)
        ref[:, width:] = sums


def tree(values):
    while len(values) > 1:
        values = [a + b for a, b in zip(values[::2], values[1::2])]
    return values[0]


def mix_tokens(tokens_ref, mix_ref, other_mix_ref, mixed_ref):
    floats = tokens_ref[...].astype(jnp.float32)
    width = floats.shape[1]
    mine = mix_ref[...].astype(jnp.float32)
    other = other_mix_ref[...].astype(jnp.float32)
    mixed_ref[...] = (floats + (mine[:, :width] + other[:, :width])).astype(jnp.bfloat16)
    return (mine[:, width : width + 1] + mine[:, width + 1 : width + 2]) + (
        other[:, width : width + 1] + other[:, width + 1 : width + 2]
    )


def sum_all(first_ref, second_ref, tokens_ref, mix_ref, other_mix_ref, *refs):
    *rows_refs, out_ref, sums_ref, mixed_ref, score_ref = refs
    score_ref[...] = jnp.broadcast_to(mix_tokens(tokens_ref, mix_ref, other_mix_ref, mixed_ref), score_ref.shape)
    width = rows_refs[0].shape[1] - sums_ref.shape[1]
    rows = jnp.concatenate([ref[:, :width].astype(jnp.float32) for ref in rows_refs], axis=0).astype(jnp.bfloat16)
    out_ref[:, :width] = mm(first_ref[...] + second_ref[...], rows, TN).astype(jnp.bfloat16)
    sums = tree([ref[:, width:].astype(jnp.float32) for ref in rows_refs])
    sums_ref[...] = sums.astype(jnp.bfloat16)
    half = out_ref.shape[1] - width
    left, right = sums[:, :half], sums[:, half:]
    if right.shape[1] < half:
        right = jnp.concatenate([right, jnp.zeros((right.shape[0], half - right.shape[1]), jnp.float32)], axis=1)
    out_ref[:, width:] = jnp.concatenate([left, right], axis=0).astype(jnp.bfloat16)


def sum_rows(first_ref, second_ref, *refs):
    *rows_refs, out_ref = refs
    rows = stack(rows_refs).astype(jnp.bfloat16)
    out_ref[...] = mm(first_ref[...] + second_ref[...], rows, TN).astype(jnp.bfloat16)


def finish(joint, tokens_ref, cotangent_ref, gain_ref, router_ref, probs_ref, inv_ref, signs_ref, back_ref, other_back_ref, *refs):
    floats = tokens_ref[...].astype(jnp.float32)
    width = floats.shape[1]
    if joint:
        score_ref, sums_ref, side_ref, corner_ref, grads_ref, router_out, gain_out = refs
        score = score_ref[:, :1]
        rows, total = sums_ref.shape
        beside = other_back_ref[:, width:].astype(jnp.float32)
        beside = jnp.concatenate([beside[:rows], beside[rows:]], axis=1)[:, :total]
        mine = sums_ref[...].astype(jnp.float32) + beside
        unpack(mine + (side_ref[...].astype(jnp.float32) + corner_ref[...].astype(jnp.float32)), router_out, gain_out)
    else:
        mix_ref, other_mix_ref, mixed_ref, grads_ref = refs
        score = mix_tokens(tokens_ref, mix_ref, other_mix_ref, mixed_ref)
    prob = probs_ref[:, :1]
    inv = inv_ref[:, :1]
    grad_first = prob * (1.0 - prob) * score
    grad_normed = back_ref[:, :width].astype(jnp.float32) + other_back_ref[:, :width].astype(jnp.float32)
    for expert in range(router_ref.shape[0]):
        column = grad_first * signs_ref[:, expert : expert + 1]
        grad_normed += column * router_ref[expert : expert + 1, :].astype(jnp.float32)
    grad_scaled = grad_normed * gain_ref[...]
    mean = jnp.mean(grad_scaled * floats, axis=1, keepdims=True)
    grads_ref[...] = (
        cotangent_ref[...].astype(jnp.float32) + inv * grad_scaled - floats * (inv * inv * inv) * mean
    ).astype(jnp.bfloat16)


def swap(value, axis):
    size = lax.axis_size(axis)
    return lax.ppermute(value, axis, [(i, i ^ 1) for i in range(size)])


def sum_over(value, axis):
    size = lax.axis_size(axis)
    if size == 1:
        return value, jnp.zeros_like(value)
    if size == 2:
        return value, swap(value, axis)
    total = lax.psum(value.astype(jnp.float32), axis)
    return total.astype(value.dtype), jnp.zeros_like(value)


def trade(blocks):
    size = len(blocks)
    pairs = [[(i, i ^ step) for i in range(size)] for step in range(size)]
    return [blocks[0]] + [lax.ppermute(blocks[step], "expert", pairs[step]) for step in range(1, size)]


def trade_whole(rows, copies):
    size = lax.axis_size("expert")
    width = rows.shape[1]
    if copies > 1:
        rows = rows.reshape(size // copies, 1, -1, width)
        rows = jnp.broadcast_to(rows, (size // copies, copies) + rows.shape[2:])
    rows = rows.reshape(size, -1, width)
    return lax.all_to_all(rows, "expert", split_axis=0, concat_axis=0, tiled=True).reshape(-1, width)


def layer(tokens, cotangent, gain, w_router, w_gate, w_up, w_down, expert_ids, slots):
    bf16, f32 = jnp.bfloat16, jnp.float32
    experts = w_router.shape[1]
    axis = lax.axis_size("expert")
    copies = axis // experts
    token_count, width = tokens.shape
    rows = 2 * token_count
    capacity = rows // experts
    hidden = w_gate.shape[2]
    parts = 2 if lax.axis_size("dp") % 2 == 0 and hidden % 256 == 0 else 1
    inner = hidden // parts
    paired = copies == 1 and axis in (2, 4, 8) and capacity % 8 == 0
    places = jnp.stack([lax.axis_index("expert"), lax.axis_index("dp") & (parts - 1)]).astype(jnp.int32)
    gain_row = gain.reshape(1, width)
    router = w_router.T
    count = axis * capacity
    all_rows = parts * count
    in_hbm = lambda value: pltpu.with_memory_space_constraint(value, pltpu.HBM)

    sends = [shape((2 * capacity, width), bf16)] * experts if paired else [shape((rows, width), bf16)] * 2
    small = shape((token_count, 128), f32)
    *blocks, first, second, probs, inv, signs, normed, tokens_here, cotangent_here, gain_here, router_here = call(
        functools.partial(prepare, experts, capacity, paired),
        (places, *(in_hbm(v) for v in (expert_ids.T, slots.T, tokens, cotangent, gain_row, router))),
        [SMEM] + [HBM] * 6,
        sends
        + [shape((rows, token_count), bf16)] * 2
        + [small, small, small, shape((token_count, width), bf16)]
        + [pltpu.VMEM((token_count, width), bf16)] * 2
        + [pltpu.VMEM((1, width), f32), pltpu.VMEM((experts, width), bf16)],
        [
            pltpu.VMEM((2, token_count), jnp.int32),
            pltpu.VMEM((2, token_count), jnp.int32),
            pltpu.SemaphoreType.DMA((6,)),
        ],
    )
    blocks = trade(blocks) if paired else [trade_whole(block, copies) for block in blocks]
    (gate_here,) = call(
        fetch,
        (places, in_hbm(w_gate[0])),
        [SMEM, HBM],
        [pltpu.VMEM((width, inner), bf16)],
        [pltpu.SemaphoreType.DMA((1,))],
        limit=1,
        flops=10**10,
        moved=2 * width * inner,
    )
    if parts == 2:
        others = [swap(block, "dp") for block in blocks]
    else:
        others = []
    if paired:
        inputs = grads = blocks + others
    else:
        inputs, grads = blocks[:1] + others[:1], blocks[1:] + others[1:]
    pieces = len(inputs)
    height = piece(inner)
    act, slope, silu, scaled, up_here = call(
        functools.partial(forward, pieces, paired),
        (places, *inputs, gain_here, gate_here, in_hbm(w_up[0])),
        [SMEM] + [VMEM] * (pieces + 2) + [HBM],
        [
            shape((all_rows, inner), bf16),
            shape((inner, all_rows), f32),
            shape((inner, all_rows), f32),
            shape((all_rows, width), f32),
            pltpu.VMEM((width, inner), bf16),
        ],
        [pltpu.SemaphoreType.DMA((inner // height,))],
        limit=4,
        flops=4 * all_rows * width * inner,
        moved=4 * width * inner,
    )
    value_shapes = [shape((count, width), f32)] + [shape((count, width), bf16)] * (parts - 1)
    *values, gate_grad, up_grad = call(
        functools.partial(middle, pieces, paired),
        (places, act, slope, silu, in_hbm(w_down[0]), *grads),
        [SMEM] + [VMEM] * 3 + [HBM] + [VMEM] * pieces,
        value_shapes + [shape((inner, all_rows), bf16)] * 2,
        [
            pltpu.VMEM((all_rows, width), f32),
            pltpu.VMEM((min(MIDDLE_FLIGHT + 1, inner // height), height, width), bf16),
            pltpu.SemaphoreType.DMA((min(MIDDLE_FLIGHT + 1, inner // height),)),
        ],
        limit=10,
        flops=4 * all_rows * width * inner,
        moved=2 * width * inner,
    )
    *backs, gain_part = call(
        backward,
        (gate_grad, up_grad, gate_here, up_here, scaled),
        [VMEM] * 5,
        value_shapes + [shape((1, width), f32)],
        flops=4 * all_rows * width * inner,
        moved=4 * width * inner,
    )
    home_shapes = [shape((capacity, width), bf16)] * experts if paired else [shape((count, width), bf16)]

    def home(pieces):
        if parts == 2:
            mine = call(add_pair, (pieces[0], swap(pieces[1], "dp")), [VMEM] * 2, home_shapes)
        else:
            mine = call(round_own, (pieces[0],), [VMEM], home_shapes)
        if paired:
            return trade(mine)
        back = trade_whole(mine[0], 1)
        if copies > 1:
            back = back.reshape(experts, copies, -1, width).astype(f32)
            back = jnp.sum(back, axis=1).reshape(-1, width).astype(bf16)
        return [back]

    axes = ("dp", "expert", "tensor")
    devices = lax.axis_size(axes)
    tiles = (experts + 1) * (width // 128)
    joint = paired and parts == 2 and capacity == 8 and lax.axis_size("tensor") == 2 and lax.axis_size("dp") == 4
    if joint:
        sums_shape = (capacity, -(-tiles // capacity) * 128)
    else:
        each = -(-tiles // devices)
        sums_shape = (devices * each, 128)
    value_rows = home(values)
    mix, sums = call(
        mix_values,
        (first, second, probs, inv, signs, normed, tokens_here, cotangent_here, router_here, gain_part, *value_rows),
        [VMEM] * (10 + len(value_rows)),
        [shape((token_count, width + 128), bf16), shape(sums_shape, f32)],
    )
    mix, other_mix = sum_over(mix, "tensor")
    last_inputs = (tokens_here, cotangent_here, gain_here, router_here, probs, inv, signs)
    token_shape = shape((token_count, width), bf16)
    router_shapes = [shape((experts, width), f32), shape((1, width), f32)]
    if joint:
        total = sums_shape[1]
        half = -(-total // 256) * 128
        other_backs = swap(backs[1], "dp")
        other_sums = swap(sums, "dp")
        mine = call(
            add_all,
            (backs[0], other_backs, sums, other_sums),
            [VMEM] * 4,
            [shape((capacity, width + total), bf16)] * experts,
        )
        back_rows = trade(mine)
        back, sums, mixed, score = call(
            sum_all,
            (first, second, tokens_here, mix, other_mix, *back_rows),
            [VMEM] * (5 + len(back_rows)),
            [shape((token_count, width + half), bf16), shape(sums_shape, bf16), token_shape, small],
        )
        other_back = swap(back, "tensor")
        side = lax.ppermute(sums, "dp", [(i, i ^ 2) for i in range(4)])
        corner = lax.ppermute(sums, ("dp", "tensor"), [(i, i ^ 5) for i in range(8)])
        grad_tokens, grad_router, grad_gain = call(
            functools.partial(finish, True),
            (*last_inputs, back, other_back, score, sums, side, corner),
            [VMEM] * 13,
            [token_shape] + router_shapes,
        )
        return (mixed, grad_tokens, grad_router.T, grad_gain.reshape(width))
    back_rows = home(backs)
    (back,) = call(
        sum_rows, (first, second, *back_rows), [VMEM] * (2 + len(back_rows)), [shape((token_count, width), bf16)]
    )
    back, other_back = sum_over(back, "tensor")
    mixed, grad_tokens = call(
        functools.partial(finish, False),
        (*last_inputs, back, other_back, mix, other_mix),
        [VMEM] * 11,
        [token_shape] * 2,
    )
    sums = sums.reshape(devices, each, 128)
    sums = lax.all_to_all(sums, axes, split_axis=0, concat_axis=0, tiled=True)
    sums = jnp.broadcast_to(jnp.sum(sums, axis=0, keepdims=True), sums.shape)
    sums = lax.all_to_all(sums, axes, split_axis=0, concat_axis=0, tiled=True)
    sums = sums.reshape(devices * each, 128)
    grad_router, grad_gain = call(gather_sums, (sums,), [VMEM], router_shapes)
    return (mixed, grad_tokens, grad_router.T, grad_gain.reshape(width))


def solution(mesh):
    return jax.shard_map(
        layer,
        mesh=mesh,
        in_specs=(
            P(("dp", "expert"), None),
            P(("dp", "expert"), None),
            P(),
            P(),
            P("expert", None, "tensor"),
            P("expert", None, "tensor"),
            P("expert", "tensor", None),
            P(("dp", "expert"), None),
            P(("dp", "expert"), None),
        ),
        out_specs=(P(("dp", "expert"), None), P(("dp", "expert"), None), P(), P()),
        check_vma=False,
    )
```

```python
import functools

import jax
import jax.numpy as jnp
from jax import lax
from jax.experimental import pallas as pl
from jax.experimental.pallas import tpu as pltpu
from jax.sharding import PartitionSpec as P


epsilon = 1e-05
MIB = 1 << 20
VMEM = pl.BlockSpec(memory_space=pltpu.VMEM)
SMEM = pl.BlockSpec(memory_space=pltpu.SMEM)
HBM = pl.BlockSpec(memory_space=pltpu.HBM)
NN = (((1,), (0,)), ((), ()))
NT = (((1,), (1,)), ((), ()))
TN = (((0,), (0,)), ((), ()))


def mm(a, b, dims):
    return lax.dot_general(a, b, dims, preferred_element_type=jnp.float32)


def shape(dims, dtype):
    return jax.ShapeDtypeStruct(dims, dtype)


def call(body, ins, in_specs, outs, scratch=(), limit=3, flops=0, moved=0):
    return pl.pallas_call(
        body,
        in_specs=in_specs,
        out_specs=[VMEM] * len(outs),
        out_shape=outs,
        scratch_shapes=scratch,
        compiler_params=pltpu.CompilerParams(vmem_limit_bytes=limit * MIB),
        cost_estimate=pl.CostEstimate(flops=flops, bytes_accessed=moved, transcendentals=0),
    )(*ins)


def piece(size):
    for width in (256, 128):
        if size % width == 0 and size > width:
            return width
    return size


def load_all(pairs, sems):
    copies = [pltpu.make_async_copy(src, dst, sems.at[i]) for i, (src, dst) in enumerate(pairs)]
    for copy in copies:
        copy.start()
    for copy in copies:
        copy.wait()


def column(row):
    size = row.shape[1]
    across = lax.broadcasted_iota(jnp.int32, (size, size), 0)
    along = lax.broadcasted_iota(jnp.int32, (size, size), 1)
    return jnp.sum(jnp.where(across == along, row, 0.0), axis=1, keepdims=True)


def prepare(experts, capacity, paired, places_ref, ids_any, slots_any, tokens_any, cotangent_any, gain_any, router_any, *refs):
    outs = refs[: experts if paired else 2]
    first_ref, second_ref, probs_ref, inv_ref, signs_ref, normed_ref = refs[len(outs) : len(outs) + 6]
    tokens_ref, cotangent_ref, gain_ref, router_ref, ids_ref, slots_ref, sems = refs[len(outs) + 6 :]
    load_all(
        (
            (ids_any, ids_ref),
            (slots_any, slots_ref),
            (tokens_any, tokens_ref),
            (cotangent_any, cotangent_ref),
            (gain_any, gain_ref),
            (router_any, router_ref),
        ),
        sems,
    )
    rows = experts * capacity
    ids = ids_ref[...]
    owner = (ids ^ places_ref[0]) if paired else ids
    index = owner * capacity + slots_ref[...]
    places = lax.broadcasted_iota(jnp.int32, (rows, index.shape[1]), 0)
    first = places == index[0:1, :]
    second = places == index[1:2, :]
    first_ref[...] = first.astype(jnp.bfloat16)
    second_ref[...] = second.astype(jnp.bfloat16)
    select = (first | second).astype(jnp.bfloat16)
    tokens = tokens_ref[...]
    inputs = mm(select, tokens, NN)
    floats = tokens.astype(jnp.float32)
    inv = lax.rsqrt(jnp.mean(floats * floats, axis=1, keepdims=True) + epsilon)
    normed = (floats * inv * gain_ref[...]).astype(jnp.bfloat16)
    logits = mm(router_ref[...], normed, NT)
    names = lax.broadcasted_iota(jnp.int32, (experts, ids.shape[1]), 0)
    signs = (names == ids[0:1, :]).astype(jnp.float32) - (names == ids[1:2, :]).astype(jnp.float32)
    prob = jax.nn.sigmoid(jnp.sum(signs * logits, axis=0, keepdims=True))
    weights = jnp.sum(jnp.where(first, prob, 0.0) + jnp.where(second, 1.0 - prob, 0.0), axis=1, keepdims=True)
    grads = weights * mm(select, cotangent_ref[...], NN)
    if paired:
        for expert, ref in enumerate(outs):
            mine = slice(expert * capacity, (expert + 1) * capacity)
            ref[...] = jnp.concatenate([inputs[mine], grads[mine]], axis=0).astype(jnp.bfloat16)
    else:
        outs[0][...] = inputs.astype(jnp.bfloat16)
        outs[1][...] = grads.astype(jnp.bfloat16)
    probs_ref[...] = jnp.broadcast_to(column(prob), probs_ref.shape)
    inv_ref[...] = jnp.broadcast_to(inv, inv_ref.shape)
    normed_ref[...] = normed
    for expert in range(experts):
        signs_ref[:, expert : expert + 1] = column(signs[expert : expert + 1, :])


def fetch(places_ref, gate_ref, up_ref, gate_out, up_out, sems):
    inner = gate_out.shape[1]
    early = up_out.shape[1]
    base = places_ref[1] * inner
    step = piece(inner)
    columns = pl.ds(pl.multiple_of(base, step), inner)
    first = pl.ds(pl.multiple_of(base, step), early)
    load_all(((gate_ref.at[:, columns], gate_out), (up_ref.at[:, first], up_out)), sems)


def stack(refs, paired=False, half=0):
    values = []
    for ref in refs:
        value = ref[...].astype(jnp.float32)
        if paired:
            rows = value.shape[0] // 2
            value = value[half * rows : (half + 1) * rows]
        values.append(value)
    return jnp.concatenate(values, axis=0)


def split(value, refs):
    rows = refs[0].shape[0]
    for place, ref in enumerate(refs):
        ref[...] = value[place * rows : (place + 1) * rows].astype(ref.dtype)


def forward(count, paired, places_ref, *refs):
    tokens_refs = refs[:count]
    gain_ref, gate_ref, first_ref, up_any = refs[count : count + 4]
    act_ref, slope_ref, silu_ref, scaled_ref, rest_ref, sems = refs[count + 4 :]
    inner = act_ref.shape[1]
    width = piece(inner)
    steps = inner // width
    early = first_ref.shape[1] // width
    base = places_ref[1] * inner

    def copy(step):
        there = pl.ds(pl.multiple_of(base + step * width, width), width)
        here = rest_ref.at[:, pl.ds((step - early) * width, width)]
        return pltpu.make_async_copy(up_any.at[:, there], here, sems.at[step - early])

    for step in range(early, steps):
        copy(step).start()
    floats = stack(tokens_refs, paired, 0)
    inv = lax.rsqrt(jnp.mean(floats * floats, axis=1, keepdims=True) + epsilon)
    scaled = floats * inv
    scaled_ref[...] = scaled
    normed = (scaled * gain_ref[...]).astype(jnp.bfloat16)
    for step in range(steps):
        span = pl.ds(step * width, width)
        gate = mm(normed, gate_ref[:, span], NN)
        if step < early:
            up = mm(normed, first_ref[:, span], NN)
        else:
            copy(step).wait()
            up = mm(normed, rest_ref[:, pl.ds((step - early) * width, width)], NN)
        sigmoid = jax.nn.sigmoid(gate)
        silu = gate * sigmoid
        act_ref[:, span] = (silu * up).astype(jnp.bfloat16)
        slope_ref[span, :] = (up * sigmoid * (1.0 + gate * (1.0 - sigmoid))).T
        silu_ref[span, :] = silu.T


def middle(count, paired, places_ref, act_ref, slope_ref, silu_ref, down_any, *refs):
    *value_refs, gate_ref, up_ref, total_ref, down_ref, sems = refs[count:]
    slots, height, _ = down_ref.shape
    inner = act_ref.shape[1]
    steps = inner // height

    def copy(step):
        there = pl.ds(pl.multiple_of(places_ref[1] * inner + step * height, height), height)
        return pltpu.make_async_copy(down_any.at[there, :], down_ref.at[step % slots], sems.at[step % slots])

    ahead = min(slots, steps) - 1
    for step in range(ahead):
        copy(step).start()
    grads = stack(refs[:count], paired, 1).T.astype(jnp.bfloat16)
    for step in range(steps):
        span = pl.ds(step * height, height)
        copy(step).wait()
        if step + ahead < steps:
            copy(step + ahead).start()
        down = down_ref.at[step % slots]
        grad_act = mm(down[...], grads, NN)
        value = mm(act_ref[:, span], down[...], NN)
        total_ref[...] = value if step == 0 else total_ref[...] + value
        gate_ref[span, :] = (grad_act * slope_ref[span, :]).astype(jnp.bfloat16)
        up_ref[span, :] = (grad_act * silu_ref[span, :]).astype(jnp.bfloat16)
    split(total_ref[...], value_refs)


def backward(gate_grad_ref, up_grad_ref, gate_ref, first_ref, rest_ref, scaled_ref, *refs):
    *value_refs, gain_ref = refs
    rows = value_refs[0].shape[0]
    height = piece(gate_ref.shape[0])
    early = first_ref.shape[1]
    for start in range(0, gate_ref.shape[0], height):
        span = pl.ds(start, height)
        back = mm(gate_ref[span, :], gate_grad_ref[...], NN) + mm(first_ref[span, :], up_grad_ref[:early, :], NN)
        back += mm(rest_ref[span, :], up_grad_ref[early:, :], NN)
        back = back.T
        for part, value_ref in enumerate(value_refs):
            value_ref[:, span] = back[part * rows : (part + 1) * rows].astype(value_ref.dtype)
        gain_ref[:, span] = jnp.sum(back * scaled_ref[:, span], axis=0, keepdims=True)


def add_pair(own_ref, other_ref, *refs):
    split(own_ref[...] + other_ref[...].astype(jnp.float32), refs)


def round_own(own_ref, *refs):
    split(own_ref[...], refs)


def mix_values(first_ref, second_ref, probs_ref, inv_ref, signs_ref, normed_ref, tokens_ref, cotangent_ref, router_ref, gain_part_ref, *refs):
    *rows_refs, mix_ref, sums_ref = refs
    rows = stack(rows_refs).astype(jnp.bfloat16)
    first = mm(first_ref[...], rows, TN)
    second = mm(second_ref[...], rows, TN)
    width = first.shape[1]
    prob = probs_ref[:, :1]
    mix_ref[:, :width] = (prob * first + (1.0 - prob) * second).astype(jnp.bfloat16)
    score = jnp.sum(cotangent_ref[...].astype(jnp.float32) * (first - second), axis=1, keepdims=True)
    coarse = score.astype(jnp.bfloat16)
    fine = (score - coarse.astype(jnp.float32)).astype(jnp.bfloat16)
    mix_ref[:, width:] = jnp.zeros((mix_ref.shape[0], mix_ref.shape[1] - width), jnp.bfloat16)
    mix_ref[:, width : width + 1] = coarse
    mix_ref[:, width + 1 : width + 2] = fine
    grad_first = prob * (1.0 - prob) * score
    normed = normed_ref[...].astype(jnp.float32)
    term = jnp.zeros(first.shape, jnp.float32)
    experts = router_ref.shape[0]
    sums = []
    for expert in range(experts):
        column = grad_first * signs_ref[:, expert : expert + 1]
        term += column * router_ref[expert : expert + 1, :].astype(jnp.float32)
        sums.append(jnp.sum(column * normed, axis=0, keepdims=True))
    scaled = tokens_ref[...].astype(jnp.float32) * inv_ref[:, :1]
    sums.append(jnp.sum(term * scaled, axis=0, keepdims=True) + gain_part_ref[...])
    spread(sums, sums_ref)


def spread(rows, out_ref):
    lanes = 128
    across = out_ref.shape[1] // lanes
    place = 0
    for row in rows:
        for start in range(0, row.shape[1], lanes):
            top, left = place // across, place % across * lanes
            out_ref[top : top + 1, left : left + lanes] = row[:, start : start + lanes]
            place += 1
    while place < out_ref.shape[0] * across:
        top, left = place // across, place % across * lanes
        out_ref[top : top + 1, left : left + lanes] = jnp.zeros((1, lanes), jnp.float32)
        place += 1


def unpack(sums, router_ref, gain_ref):
    lanes = 128
    across = sums.shape[1] // lanes
    steps = gain_ref.shape[1] // lanes
    experts = router_ref.shape[0]
    for expert in range(experts + 1):
        out_ref, row = (router_ref, expert) if expert < experts else (gain_ref, 0)
        for step in range(steps):
            place = expert * steps + step
            top, left = place // across, place % across * lanes
            value = sums[top : top + 1, left : left + lanes]
            out_ref[row : row + 1, step * lanes : (step + 1) * lanes] = value


def gather_sums(sums_ref, router_ref, gain_ref):
    unpack(sums_ref, router_ref, gain_ref)


def add_all(own_ref, other_ref, sums_ref, other_sums_ref, *refs):
    rows = refs[0].shape[0]
    width = own_ref.shape[1]
    total = own_ref[...] + other_ref[...].astype(jnp.float32)
    sums = (sums_ref[...] + other_sums_ref[...]).astype(jnp.bfloat16)
    for place, ref in enumerate(refs):
        ref[:, :width] = total[place * rows : (place + 1) * rows].astype(jnp.bfloat16)
        ref[:, width:] = sums


def tree(values):
    while len(values) > 1:
        values = [a + b for a, b in zip(values[::2], values[1::2])]
    return values[0]


def mix_tokens(tokens_ref, mix_ref, other_mix_ref, mixed_ref):
    floats = tokens_ref[...].astype(jnp.float32)
    width = floats.shape[1]
    mine = mix_ref[...].astype(jnp.float32)
    other = other_mix_ref[...].astype(jnp.float32)
    mixed_ref[...] = (floats + (mine[:, :width] + other[:, :width])).astype(jnp.bfloat16)
    return (mine[:, width : width + 1] + mine[:, width + 1 : width + 2]) + (
        other[:, width : width + 1] + other[:, width + 1 : width + 2]
    )


def sum_all(first_ref, second_ref, tokens_ref, mix_ref, other_mix_ref, *refs):
    *rows_refs, out_ref, sums_ref, mixed_ref, score_ref = refs
    score_ref[...] = jnp.broadcast_to(mix_tokens(tokens_ref, mix_ref, other_mix_ref, mixed_ref), score_ref.shape)
    width = rows_refs[0].shape[1] - sums_ref.shape[1]
    rows = jnp.concatenate([ref[:, :width].astype(jnp.float32) for ref in rows_refs], axis=0).astype(jnp.bfloat16)
    out_ref[:, :width] = mm(first_ref[...] + second_ref[...], rows, TN).astype(jnp.bfloat16)
    sums = tree([ref[:, width:].astype(jnp.float32) for ref in rows_refs])
    sums_ref[...] = sums.astype(jnp.bfloat16)
    half = out_ref.shape[1] - width
    left, right = sums[:, :half], sums[:, half:]
    if right.shape[1] < half:
        right = jnp.concatenate([right, jnp.zeros((right.shape[0], half - right.shape[1]), jnp.float32)], axis=1)
    out_ref[:, width:] = jnp.concatenate([left, right], axis=0).astype(jnp.bfloat16)


def sum_rows(first_ref, second_ref, *refs):
    *rows_refs, out_ref = refs
    rows = stack(rows_refs).astype(jnp.bfloat16)
    out_ref[...] = mm(first_ref[...] + second_ref[...], rows, TN).astype(jnp.bfloat16)


def finish(joint, tokens_ref, cotangent_ref, gain_ref, router_ref, probs_ref, inv_ref, signs_ref, back_ref, other_back_ref, *refs):
    floats = tokens_ref[...].astype(jnp.float32)
    width = floats.shape[1]
    if joint:
        score_ref, sums_ref, side_ref, corner_ref, grads_ref, router_out, gain_out = refs
        score = score_ref[:, :1]
        rows, total = sums_ref.shape
        beside = other_back_ref[:, width:].astype(jnp.float32)
        beside = jnp.concatenate([beside[:rows], beside[rows:]], axis=1)[:, :total]
        mine = sums_ref[...].astype(jnp.float32) + beside
        unpack(mine + (side_ref[...].astype(jnp.float32) + corner_ref[...].astype(jnp.float32)), router_out, gain_out)
    else:
        mix_ref, other_mix_ref, mixed_ref, grads_ref = refs
        score = mix_tokens(tokens_ref, mix_ref, other_mix_ref, mixed_ref)
    prob = probs_ref[:, :1]
    inv = inv_ref[:, :1]
    grad_first = prob * (1.0 - prob) * score
    grad_normed = back_ref[:, :width].astype(jnp.float32) + other_back_ref[:, :width].astype(jnp.float32)
    for expert in range(router_ref.shape[0]):
        column = grad_first * signs_ref[:, expert : expert + 1]
        grad_normed += column * router_ref[expert : expert + 1, :].astype(jnp.float32)
    grad_scaled = grad_normed * gain_ref[...]
    mean = jnp.mean(grad_scaled * floats, axis=1, keepdims=True)
    grads_ref[...] = (
        cotangent_ref[...].astype(jnp.float32) + inv * grad_scaled - floats * (inv * inv * inv) * mean
    ).astype(jnp.bfloat16)


def swap(value, axis):
    size = lax.axis_size(axis)
    return lax.ppermute(value, axis, [(i, i ^ 1) for i in range(size)])


def sum_over(value, axis):
    size = lax.axis_size(axis)
    if size == 1:
        return value, jnp.zeros_like(value)
    if size == 2:
        return value, swap(value, axis)
    total = lax.psum(value.astype(jnp.float32), axis)
    return total.astype(value.dtype), jnp.zeros_like(value)


def trade(blocks):
    size = len(blocks)
    pairs = [[(i, i ^ step) for i in range(size)] for step in range(size)]
    return [blocks[0]] + [lax.ppermute(blocks[step], "expert", pairs[step]) for step in range(1, size)]


def trade_whole(rows, copies):
    size = lax.axis_size("expert")
    width = rows.shape[1]
    if copies > 1:
        rows = rows.reshape(size // copies, 1, -1, width)
        rows = jnp.broadcast_to(rows, (size // copies, copies) + rows.shape[2:])
    rows = rows.reshape(size, -1, width)
    return lax.all_to_all(rows, "expert", split_axis=0, concat_axis=0, tiled=True).reshape(-1, width)


def layer(tokens, cotangent, gain, w_router, w_gate, w_up, w_down, expert_ids, slots):
    bf16, f32 = jnp.bfloat16, jnp.float32
    experts = w_router.shape[1]
    axis = lax.axis_size("expert")
    copies = axis // experts
    token_count, width = tokens.shape
    rows = 2 * token_count
    capacity = rows // experts
    hidden = w_gate.shape[2]
    parts = 2 if lax.axis_size("dp") % 2 == 0 and hidden % 256 == 0 else 1
    inner = hidden // parts
    paired = copies == 1 and axis in (2, 4, 8) and capacity % 8 == 0
    places = jnp.stack([lax.axis_index("expert"), lax.axis_index("dp") & (parts - 1)]).astype(jnp.int32)
    gain_row = gain.reshape(1, width)
    router = w_router.T
    count = axis * capacity
    all_rows = parts * count
    in_hbm = lambda value: pltpu.with_memory_space_constraint(value, pltpu.HBM)

    sends = [shape((2 * capacity, width), bf16)] * experts if paired else [shape((rows, width), bf16)] * 2
    small = shape((token_count, 128), f32)
    *blocks, first, second, probs, inv, signs, normed, tokens_here, cotangent_here, gain_here, router_here = call(
        functools.partial(prepare, experts, capacity, paired),
        (places, *(in_hbm(v) for v in (expert_ids.T, slots.T, tokens, cotangent, gain_row, router))),
        [SMEM] + [HBM] * 6,
        sends
        + [shape((rows, token_count), bf16)] * 2
        + [small, small, small, shape((token_count, width), bf16)]
        + [pltpu.VMEM((token_count, width), bf16)] * 2
        + [pltpu.VMEM((1, width), f32), pltpu.VMEM((experts, width), bf16)],
        [
            pltpu.VMEM((2, token_count), jnp.int32),
            pltpu.VMEM((2, token_count), jnp.int32),
            pltpu.SemaphoreType.DMA((6,)),
        ],
    )
    blocks = trade(blocks) if paired else [trade_whole(block, copies) for block in blocks]
    height = piece(inner)
    early = max(1, inner // height * 2 // 3) * height
    gate_here, up_first = call(
        fetch,
        (places, in_hbm(w_gate[0]), in_hbm(w_up[0])),
        [SMEM, HBM, HBM],
        [pltpu.VMEM((width, inner), bf16), pltpu.VMEM((width, early), bf16)],
        [pltpu.SemaphoreType.DMA((2,))],
        limit=1,
        flops=10**10,
        moved=2 * width * inner,
    )
    if parts == 2:
        others = [swap(block, "dp") for block in blocks]
    else:
        others = []
    if paired:
        inputs = grads = blocks + others
    else:
        inputs, grads = blocks[:1] + others[:1], blocks[1:] + others[1:]
    pieces = len(inputs)
    act, slope, silu, scaled, up_rest = call(
        functools.partial(forward, pieces, paired),
        (places, *inputs, gain_here, gate_here, up_first, in_hbm(w_up[0])),
        [SMEM] + [VMEM] * (pieces + 3) + [HBM],
        [
            shape((all_rows, inner), bf16),
            shape((inner, all_rows), f32),
            shape((inner, all_rows), f32),
            shape((all_rows, width), f32),
            pltpu.VMEM((width, inner - early), bf16),
        ],
        [pltpu.SemaphoreType.DMA(((inner - early) // height,))],
        limit=4,
        flops=4 * all_rows * width * inner,
        moved=4 * width * inner,
    )
    value_shapes = [shape((count, width), f32)] + [shape((count, width), bf16)] * (parts - 1)
    *values, gate_grad, up_grad = call(
        functools.partial(middle, pieces, paired),
        (places, act, slope, silu, in_hbm(w_down[0]), *grads),
        [SMEM] + [VMEM] * 3 + [HBM] + [VMEM] * pieces,
        value_shapes + [shape((inner, all_rows), bf16)] * 2,
        [
            pltpu.VMEM((all_rows, width), f32),
            pltpu.VMEM((min(4, inner // height), height, width), bf16),
            pltpu.SemaphoreType.DMA((min(4, inner // height),)),
        ],
        limit=10,
        flops=4 * all_rows * width * inner,
        moved=2 * width * inner,
    )
    *backs, gain_part = call(
        backward,
        (gate_grad, up_grad, gate_here, up_first, up_rest, scaled),
        [VMEM] * 6,
        value_shapes + [shape((1, width), f32)],
        flops=4 * all_rows * width * inner,
        moved=4 * width * inner,
    )
    home_shapes = [shape((capacity, width), bf16)] * experts if paired else [shape((count, width), bf16)]

    def home(pieces):
        if parts == 2:
            mine = call(add_pair, (pieces[0], swap(pieces[1], "dp")), [VMEM] * 2, home_shapes)
        else:
            mine = call(round_own, (pieces[0],), [VMEM], home_shapes)
        if paired:
            return trade(mine)
        back = trade_whole(mine[0], 1)
        if copies > 1:
            back = back.reshape(experts, copies, -1, width).astype(f32)
            back = jnp.sum(back, axis=1).reshape(-1, width).astype(bf16)
        return [back]

    axes = ("dp", "expert", "tensor")
    devices = lax.axis_size(axes)
    tiles = (experts + 1) * (width // 128)
    joint = paired and parts == 2 and capacity == 8 and lax.axis_size("tensor") == 2 and lax.axis_size("dp") == 4
    if joint:
        sums_shape = (capacity, -(-tiles // capacity) * 128)
    else:
        each = -(-tiles // devices)
        sums_shape = (devices * each, 128)
    value_rows = home(values)
    mix, sums = call(
        mix_values,
        (first, second, probs, inv, signs, normed, tokens_here, cotangent_here, router_here, gain_part, *value_rows),
        [VMEM] * (10 + len(value_rows)),
        [shape((token_count, width + 128), bf16), shape(sums_shape, f32)],
    )
    mix, other_mix = sum_over(mix, "tensor")
    last_inputs = (tokens_here, cotangent_here, gain_here, router_here, probs, inv, signs)
    token_shape = shape((token_count, width), bf16)
    router_shapes = [shape((experts, width), f32), shape((1, width), f32)]
    if joint:
        total = sums_shape[1]
        half = -(-total // 256) * 128
        other_backs = swap(backs[1], "dp")
        other_sums = swap(sums, "dp")
        mine = call(
            add_all,
            (backs[0], other_backs, sums, other_sums),
            [VMEM] * 4,
            [shape((capacity, width + total), bf16)] * experts,
        )
        back_rows = trade(mine)
        back, sums, mixed, score = call(
            sum_all,
            (first, second, tokens_here, mix, other_mix, *back_rows),
            [VMEM] * (5 + len(back_rows)),
            [shape((token_count, width + half), bf16), shape(sums_shape, bf16), token_shape, small],
        )
        other_back = swap(back, "tensor")
        side = lax.ppermute(sums, "dp", [(i, i ^ 2) for i in range(4)])
        corner = lax.ppermute(sums, ("dp", "tensor"), [(i, i ^ 5) for i in range(8)])
        grad_tokens, grad_router, grad_gain = call(
            functools.partial(finish, True),
            (*last_inputs, back, other_back, score, sums, side, corner),
            [VMEM] * 13,
            [token_shape] + router_shapes,
        )
        return (mixed, grad_tokens, grad_router.T, grad_gain.reshape(width))
    back_rows = home(backs)
    (back,) = call(
        sum_rows, (first, second, *back_rows), [VMEM] * (2 + len(back_rows)), [shape((token_count, width), bf16)]
    )
    back, other_back = sum_over(back, "tensor")
    mixed, grad_tokens = call(
        functools.partial(finish, False),
        (*last_inputs, back, other_back, mix, other_mix),
        [VMEM] * 11,
        [token_shape] * 2,
    )
    sums = sums.reshape(devices, each, 128)
    sums = lax.all_to_all(sums, axes, split_axis=0, concat_axis=0, tiled=True)
    sums = jnp.broadcast_to(jnp.sum(sums, axis=0, keepdims=True), sums.shape)
    sums = lax.all_to_all(sums, axes, split_axis=0, concat_axis=0, tiled=True)
    sums = sums.reshape(devices * each, 128)
    grad_router, grad_gain = call(gather_sums, (sums,), [VMEM], router_shapes)
    return (mixed, grad_tokens, grad_router.T, grad_gain.reshape(width))


def solution(mesh):
    return jax.shard_map(
        layer,
        mesh=mesh,
        in_specs=(
            P(("dp", "expert"), None),
            P(("dp", "expert"), None),
            P(),
            P(),
            P("expert", None, "tensor"),
            P("expert", None, "tensor"),
            P("expert", "tensor", None),
            P(("dp", "expert"), None),
            P(("dp", "expert"), None),
        ),
        out_specs=(P(("dp", "expert"), None), P(("dp", "expert"), None), P(), P()),
        check_vma=False,
    )
```
